256 devices in a mesh: img: 16 (over y, x_hi, core), ori: 8 (over z), slab: 2 (over x_lo).
Axes of the slice: x: 4 (x_hi: 2, x_lo: 2; x = x_hi * 2 + x_lo), y: 4, z: 8, core: 2. Of those that a mesh axis runs over, the one named last changes fastest.
Arguments:
- images: bfloat16 [3072, 160, 256], P('img', 'slab'), may hold values from -6 to 6
- noise_weight: float32 [160, 128], P('slab'), may hold values from 0.5 to 200
- prior_mask: int32 [3072, 1536], P('img', 'ori'), may hold values from 0 to 1, as said below
- volume: bfloat16 [128, 4, 256], P(None, 'slab'), may hold values from -0.046875 to 0.046875
- interp_weights: bfloat16 [1536, 96, 512], P(('ori', 'img'), None, 'slab'), may hold values from -1.5 to 1.5
- row_first: int32 [1536, 2], P(('ori', 'img'), 'slab'), may hold values from 0 to 112, as said below
- row_count: int32 [1536, 2], P(('ori', 'img'), 'slab'), may hold values from 48 to 96, as said below
Outputs:
- log_evidence: float32 [3072], P('img')
- inserted: float32 [128, 4, 256], P(('img', 'ori'), 'slab')
The draws below stay inside these ranges and needn't reach their ends.
Inputs may be any that keep to these rules, and one draw needn't show every extreme that they name: `prior_mask`: every image allows at least one orientation. row_first + row_count <= 160. `row_count`: the first slice reaches 96 rows on every slab.
All inputs are finite; a program needn't handle non-finite values.
Results may differ from the reference program's by a relative error of at most 0.013.
Values may be sent and summed in bfloat16 or wider, within the bound.
No kernel may reach another device: no remote copies, remote signals or barrier semaphores. Data moves between devices by JAX's collectives and lax.ppermute only.
A program may use at most 128 MiB of HBM per device.

```python
import jax
import jax.numpy as jnp
from jax import lax

ROWS = 160
LINE = 128
VY = 128
RB = 96
IMG_DEV = 192
PS = 2
ORIENT = 1536
IMAGES = 3072
LINES_DEV = 256
PLANES = 4
N_IMG = 16
N_SLAB = 2


def row_spans(key):
    base = jax.random.fold_in(key, 11)
    counts = jax.random.randint(jax.random.fold_in(base, 1), (ORIENT, N_SLAB), RB // 2, RB + 1)
    counts = counts.at[0].set(RB)
    starts = jax.random.randint(jax.random.fold_in(base, 2), (ORIENT, N_SLAB), 0, ROWS - counts + 1)
    return (starts.astype(jnp.int32), counts.astype(jnp.int32))


def draw_row_first(key, part):
    return row_spans(key)[0]


def draw_row_count(key, part):
    return row_spans(key)[1]


def draw_prior_mask(key, part):
    random_bits = jax.random.randint(jax.random.fold_in(key, 21), (IMAGES, ORIENT), 0, 2)
    chosen = jax.random.randint(jax.random.fold_in(key, 22), (IMAGES,), 0, ORIENT)
    forced = (jnp.arange(ORIENT)[None, :] == chosen[:, None]).astype(jnp.int32)
    return jnp.maximum(random_bits, forced).astype(jnp.int32)


def draw_noise_weight(key, part):
    even = jax.random.uniform(jax.random.fold_in(key, 31), (ROWS, LINE), jnp.float32)
    return jnp.exp(jnp.log(0.5) + even * jnp.log(4.0)).astype(jnp.float32)


def strengthened(entries, key, source, target, blocks, factor):
    def block_of(dim):
        return (jnp.arange(entries.shape[dim]) // (entries.shape[dim] // blocks)).reshape((-1,) + (1,) * (entries.ndim - 1 - dim))

    first = jax.random.permutation(key, blocks)[block_of(target)]
    other_side = (block_of(target) + blocks // 2) % blocks
    return jnp.where((block_of(source) == first) | (block_of(source) == other_side), factor * entries, entries)


def level_of(key, extent, shards, least, largest):
    gain = 1.0
    for position, shards_of in shards:
        heights = jax.random.uniform(jax.random.fold_in(jax.random.fold_in(key, 6), position), (shards_of,), jnp.float32, least / len(shards), largest / len(shards))
        gain = gain * jnp.repeat(jnp.exp(heights), extent[position] // shards_of).reshape((-1,) + (1,) * (len(extent) - 1 - position))
    return gain


def centred(own_key, extent, spread, most, pieces=(), dtype=jnp.bfloat16):
    loudness = level_of(own_key, extent, pieces, -0.22, 0.18) if pieces else 1.0
    entries = jax.random.normal(own_key, extent, jnp.float32) * spread * loudness
    return jnp.minimum(jnp.maximum(entries, -most), most).astype(dtype)


def gaussian_with(key, shape, spread, most, split, heavy, kind=jnp.bfloat16):
    drawn = spread * jax.random.normal(key, shape, jnp.float32)
    if split:
        drawn = drawn * level_of(key, shape, split, -0.22, 0.18)
    return jnp.clip(strengthened(drawn, jax.random.fold_in(key, 3), *heavy), -most, most).astype(kind)


def setup_inputs(seed: int = 0) -> dict:
    streams_of = jax.random.split(jax.random.key(seed), 8)
    return {
        "images": centred(streams_of[0], (IMAGES, ROWS, 2 * LINE), 1.0, 6.0, ((0, 16), (1, 2))),
        "noise_weight": draw_noise_weight(jax.random.fold_in(streams_of[7], 71), 0),
        "prior_mask": draw_prior_mask(jax.random.fold_in(streams_of[7], 71), 0),
        "volume": centred(streams_of[3], (VY, PLANES, 2 * LINE), (1.2 / (ROWS * LINE) ** 0.5), 0.046875, ((1, 2),)),
        "interp_weights": gaussian_with(streams_of[4], (ORIENT, RB, N_SLAB * LINES_DEV), LINES_DEV ** -0.5, 1.5, ((0, 128), (2, 2)), (0, 2, 128, 5.5)),
        "row_first": draw_row_first(jax.random.fold_in(streams_of[7], 71), 0),
        "row_count": draw_row_count(jax.random.fold_in(streams_of[7], 71), 0),
    }


def place_rows(block, row_start):
    padded = jnp.zeros((ROWS + RB, block.shape[1]), jnp.float32)
    updated = lax.dynamic_update_slice(padded, block, (row_start.astype(jnp.int32), jnp.int32(0)))
    return updated[:ROWS]


def pick_rows(source, row_start):
    return lax.dynamic_slice_in_dim(source, row_start.astype(jnp.int32), RB, 0)


def reference(images, noise_weight, prior_mask, volume, interp_weights, row_first, row_count):
    line_count = VY * PS
    width = 2 * LINE
    partial_sum = jnp.zeros((ORIENT, ROWS, width), jnp.float32)
    for slab in range(N_SLAB):
        kept_rows = (jnp.arange(RB)[None, :] < row_count[:, slab][:, None]).astype(jnp.float32)
        vol_lines = volume[:, slab * PS:(slab + 1) * PS, :].reshape(line_count, width).astype(jnp.float32)
        weights_f = interp_weights[:, :, slab * line_count:(slab + 1) * line_count].astype(jnp.float32)
        blocks = jnp.einsum('ojl,lc->ojc', weights_f, vol_lines) * kept_rows[:, :, None]
        partial_sum = partial_sum + jax.vmap(place_rows)(blocks, row_first[:, slab])
    slices = partial_sum.astype(jnp.bfloat16)
    noise_both = jnp.concatenate([noise_weight, noise_weight], axis=1)
    slice_float = slices.astype(jnp.float32)
    weighted = (noise_both[None] * slice_float).astype(jnp.bfloat16)
    flat_images = images.reshape(IMAGES, ROWS * width)
    inner_prod = jnp.dot(flat_images, weighted.reshape(ORIENT, ROWS * width).T, preferred_element_type=jnp.float32)
    quadratic = 0.5 * jnp.sum(noise_both[None] * slice_float * slice_float, axis=(1, 2))
    scores = inner_prod - quadratic[None, :]
    allowed = prior_mask > 0
    highest = jnp.max(jnp.where(allowed, scores, -1e30), axis=1)
    exp_scores = jnp.where(allowed, jnp.exp(scores - highest[:, None]), 0.0)
    total_mass = jnp.sum(exp_scores, axis=1)
    log_evidence = highest + jnp.log(total_mass)
    posterior = (exp_scores / total_mass[:, None]).astype(jnp.bfloat16)
    image_blocks = flat_images.reshape(N_IMG, IMG_DEV, ROWS * width)
    post_blocks = posterior.reshape(N_IMG, IMG_DEV, ORIENT)

    def add_block(carried, pair):
        part_sum = jnp.dot(pair[1].T, pair[0], preferred_element_type=jnp.float32).astype(jnp.bfloat16)
        part_sum = lax.optimization_barrier(part_sum)
        return carried + part_sum.astype(jnp.float32), None

    summed, unused = lax.scan(add_block, jnp.zeros((ORIENT, ROWS * width), jnp.float32), (image_blocks, post_blocks))
    image_sums = summed.astype(jnp.bfloat16).reshape(ORIENT, ROWS, width)
    padded = jnp.pad(image_sums, ((0, 0), (0, RB), (0, 0)))
    outputs = []
    for slab in range(N_SLAB):
        kept_rows = (jnp.arange(RB)[None, :] < row_count[:, slab][:, None]).astype(jnp.float32)
        picked = jax.vmap(pick_rows)(padded, row_first[:, slab]).astype(jnp.float32) * kept_rows[:, :, None]
        weights_f = interp_weights[:, :, slab * line_count:(slab + 1) * line_count].astype(jnp.float32)
        accumulated = jnp.einsum('ojl,ojc->lc', weights_f, picked)
        outputs.append(accumulated.reshape(VY, PS, width))
    inserted = jnp.concatenate(outputs, axis=1)
    return log_evidence, inserted
```

```python
import jax
import jax.numpy as jnp
from jax import lax
from jax.experimental import pallas as pl
from jax.experimental.pallas import tpu as pltpu
from jax.sharding import Mesh
from jax.sharding import PartitionSpec as P

IMG = ("y", "xh", "core")
BF16 = jnp.bfloat16
F32 = jnp.float32
SOURCES = ((0, 0), (0, 1), (-1, 0), (1, 0), (-1, 1), (1, 1), (2, 0), (2, 1))


def shifted(x, axis, step):
    n = lax.axis_size(axis)
    return lax.ppermute(x, axis, [(i, (i + step) % n) for i in range(n)])


def gathered(near, far):
    beside = shifted(near, "xh", 1)
    up = shifted(near, "y", 1)
    down = shifted(near, "y", -1)
    far = shifted(far, "slab", 1)
    across = shifted(up, "y", 1)
    beside_down = shifted(beside, "y", -1)
    beside_up = shifted(beside, "y", 1)
    far_beside = shifted(far, "xh", 1)
    far_down = shifted(far, "y", -1)
    far_up = shifted(far, "y", 1)
    far_across = shifted(far_down, "y", -1)
    far_beside_down = shifted(far_beside, "y", -1)
    far_beside_up = shifted(far_beside, "y", 1)
    across_beside = shifted(across, "xh", 1)
    far_across_beside = shifted(far_across, "xh", 1)
    return (
        [near, beside, up, down, beside_up, beside_down, across, across_beside],
        [far, far_beside, far_up, far_down, far_beside_up, far_beside_down, far_across, far_across_beside],
    )


def placed_rows(weights, row_first, row_count, half, half_rows):
    owned, reach, _ = weights.shape
    row = lax.broadcasted_iota(jnp.int32, (owned, half_rows, reach), 1)
    entry = lax.broadcasted_iota(jnp.int32, (owned, half_rows, reach), 2)
    at = half * half_rows + row - row_first[:, :, None]
    chosen = (entry == at) & (entry < row_count[:, :, None])
    return jnp.einsum("orj,ojl->orl", chosen.astype(BF16), weights, preferred_element_type=BF16)


def column_choice(total, owned, core):
    my_y = lax.axis_index("y")
    my_x = lax.axis_index("xh")
    picks = []
    for dy, dx in SOURCES:
        chip = ((my_y + dy + 4) % 4) * 2 + (my_x + dx) % 2
        first = (chip * 2 + core) * owned
        picks.append(first + jnp.arange(owned))
    wanted = jnp.concatenate(picks)
    return (jnp.arange(total)[None, :] == wanted[:, None]).astype(BF16)


def weighted_kernel(*refs):
    chips = (len(refs) - 6) // 2
    near, far = refs[:chips], refs[chips : 2 * chips]
    lines, lines_far, noise, out, quad, wide = refs[2 * chips :]
    rows = out.shape[0]
    step = noise.shape[0]
    some = step // rows
    owned = near[0].shape[0] // rows
    for chip in range(chips):

        def project(i, carry, chip=chip):
            at = pl.multiple_of(i * step, step)
            slices = jnp.dot(near[chip][pl.ds(at, step), :], lines[...], preferred_element_type=F32)
            slices += jnp.dot(far[chip][pl.ds(at, step), :], lines_far[...], preferred_element_type=F32)
            slices = slices.astype(BF16).astype(F32)
            weighted = noise[...] * slices
            wide[0, pl.ds(pl.multiple_of(chip * owned * rows + i * step, step), step), :] = weighted[:, :128]
            wide[1, pl.ds(pl.multiple_of(chip * owned * rows + i * step, step), step), :] = weighted[:, 128:]
            square = weighted * slices
            square = square[:, :128] + square[:, 128:]
            quad[pl.ds(chip * owned + i * some, some)] = jnp.sum(
                square.reshape(some, rows // 8, 8, 128), axis=1
            )
            return carry

        lax.fori_loop(0, owned // some, project, 0)

    def turn(r, carry):
        for half in range(2):
            out[r, :, half * 128 : half * 128 + 128] = wide[
                half, pl.ds(r, chips * owned, stride=rows), :
            ].astype(BF16)
        return carry

    lax.fori_loop(0, rows, turn, 0, unroll=4)


def weighted_slices(near, far, lines, lines_far, noise, rows):
    chips = len(near)
    count = chips * near[0].shape[0] // rows
    width = lines.shape[1]
    return pl.pallas_call(
        weighted_kernel,
        out_shape=(
            jax.ShapeDtypeStruct((rows, count, width), BF16),
            jax.ShapeDtypeStruct((count, 8, 128), F32),
        ),
        scratch_shapes=[pltpu.VMEM((2, count * rows, 128), F32)],
        compiler_params=pltpu.CompilerParams(vmem_limit_bytes=40 << 20),
        name="weighted_slices",
    )(*near, *far, lines, lines_far, noise)


def score_kernel(first, second, quad_first, quad_second, own, beside, out, acc):
    step = pl.program_id(0)
    rows = own.shape[0]
    shots = own.shape[1]

    @pl.when(step == 0)
    def _():
        acc[...] = jnp.zeros_like(acc)

    slices = jnp.concatenate(
        [jnp.concatenate([first[r], second[r]], axis=0) for r in range(rows)], axis=1
    )
    for k, shot in enumerate((own, beside)):
        block = jnp.concatenate([shot[r] for r in range(rows)], axis=1)
        acc[k] += lax.dot_general(
            slices, block, (((1,), (1,)), ((), ())), preferred_element_type=F32
        )

    @pl.when(step == pl.num_programs(0) - 1)
    def _():
        quad = jnp.concatenate([jnp.sum(quad_first[...], axis=1), jnp.sum(quad_second[...], axis=1)], axis=0)
        half = 0.5 * jnp.sum(quad, axis=1, keepdims=True)
        out[:, :shots] = acc[0] - half
        out[:, shots:] = acc[1] - half


def partial_scores(first, second, quad_first, quad_second, own, beside, block=8):
    rows, shots, width = own.shape
    count = first.shape[1]
    slices_spec = pl.BlockSpec((block, count, width), lambda i: (i, 0, 0))
    quad_spec = pl.BlockSpec(quad_first.shape, lambda i: (0, 0, 0))
    shots_spec = pl.BlockSpec((block, shots, width), lambda i: (i, 0, 0))
    return pl.pallas_call(
        score_kernel,
        grid=(rows // block,),
        in_specs=[slices_spec, slices_spec, quad_spec, quad_spec, shots_spec, shots_spec],
        out_specs=pl.BlockSpec((2 * count, 2 * shots), lambda i: (0, 0)),
        out_shape=jax.ShapeDtypeStruct((2 * count, 2 * shots), F32),
        scratch_shapes=[pltpu.VMEM((2, 2 * count, shots), F32)],
        compiler_params=pltpu.CompilerParams(
            dimension_semantics=("arbitrary",), vmem_limit_bytes=40 << 20
        ),
        name="partial_scores",
    )(first, second, quad_first, quad_second, own, beside)


def rows_major_kernel(shots, out, wide):
    count, rows, _ = shots.shape

    def spread(n, carry):
        block = shots[n].astype(F32)
        at = pl.multiple_of(n * rows, rows)
        wide[0, pl.ds(at, rows), :] = block[:, :128]
        wide[1, pl.ds(at, rows), :] = block[:, 128:]
        return carry

    lax.fori_loop(0, count, spread, 0, unroll=4)

    def turn(r, carry):
        for half in range(2):
            out[r, :, half * 128 : half * 128 + 128] = wide[
                half, pl.ds(r, count, stride=rows), :
            ].astype(BF16)
        return carry

    lax.fori_loop(0, rows, turn, 0, unroll=8)


def rows_major(images, block=32):
    shots, rows, width = images.shape
    return pl.pallas_call(
        rows_major_kernel,
        grid=(shots // block,),
        in_specs=[pl.BlockSpec((block, rows, width), lambda i: (i, 0, 0))],
        out_specs=pl.BlockSpec((rows, block, width), lambda i: (0, i, 0)),
        out_shape=jax.ShapeDtypeStruct((rows, shots, width), BF16),
        scratch_shapes=[pltpu.VMEM((2, block * rows, 128), F32)],
        compiler_params=pltpu.CompilerParams(
            dimension_semantics=("arbitrary",), vmem_limit_bytes=20 << 20
        ),
        name="rows_major",
    )(images)


def turn_kernel(*refs):
    chunks, out, flat = refs[:-2], refs[-2], refs[-1]
    half = len(chunks) // 2
    size, lines = chunks[0].shape
    for side in range(2):
        for i in range(half):
            flat[side, i * size : (i + 1) * size, :] = chunks[side * half + i][...]
    for side in range(2):

        def turn(i, carry, side=side):
            at = pl.multiple_of(i * 128, 128)
            out[side * lines : (side + 1) * lines, pl.ds(at, 128)] = flat[side, pl.ds(at, 128), :].T
            return carry

        lax.fori_loop(0, half * size // 128, turn, 0, unroll=2)


def turned_weights(near, far):
    size, lines = near[0].shape
    span = len(near) * size
    return pl.pallas_call(
        turn_kernel,
        out_shape=jax.ShapeDtypeStruct((2 * lines, span), BF16),
        scratch_shapes=[pltpu.VMEM((2, span, lines), BF16)],
        compiler_params=pltpu.CompilerParams(vmem_limit_bytes=20 << 20),
        name="turned_weights",
    )(*near, *far)


def insert_kernel(
    slab, scores, allowed, stats, own, beside, turned, turned_too, out, post_own, post_beside, wide, flat, here, done
):
    step = pl.program_id(0)
    rows = own.shape[0]
    shots = own.shape[1]
    all_rows = rows * pl.num_programs(0)
    count = scores.shape[0]
    lines = out.shape[1]
    fetches = [
        pltpu.make_async_copy(turned, here.at[0], done.at[0]),
        pltpu.make_async_copy(turned_too, here.at[1], done.at[1]),
    ]

    @pl.when(step == 0)
    def _():
        for fetch in fetches:
            fetch.start()
        mass = jnp.exp(scores[...] - stats[0:1, :])
        post = jnp.where(allowed[...] > 0.5, mass, 0.0) / stats[1:2, :]
        post_own[...] = post[:, :shots].astype(BF16)
        post_beside[...] = post[:, shots:].astype(BF16)

    for r in range(rows):
        sums = jnp.dot(post_own[...], own[r], preferred_element_type=F32)
        sums += jnp.dot(post_beside[...], beside[r], preferred_element_type=F32)
        for half in range(2):
            wide[half, pl.ds(step * rows + r, count, stride=all_rows), :] = sums[
                :, half * 128 : half * 128 + 128
            ]

    @pl.when(step == pl.num_programs(0) - 1)
    def _():
        span = 640

        def narrow(i, carry):
            at = pl.multiple_of(i * span, span)
            for half in range(2):
                flat[pl.ds(at, span), half * 128 : half * 128 + 128] = wide[
                    half, pl.ds(at, span), :
                ].astype(BF16)
            return carry

        lax.fori_loop(0, count * all_rows // span, narrow, 0)
        for fetch in fetches:
            fetch.wait()
        split = count * all_rows // 2
        for side, slot in ((0, slab[0]), (1, 1 - slab[0])):
            total = jnp.dot(
                here[0, side * lines : (side + 1) * lines, :], flat[:split, :], preferred_element_type=F32
            )
            total += jnp.dot(
                here[1, side * lines : (side + 1) * lines, :], flat[split:, :], preferred_element_type=F32
            )
            out[slot] = total.astype(BF16)


def insertion(slab, scores, allowed, stats, own, beside, turned, turned_too, block=8):
    rows, shots, width = own.shape
    count = scores.shape[0]
    lines = turned.shape[0] // 2
    whole = lambda x: pl.BlockSpec(x.shape, lambda i, s: (0, 0))
    shots_spec = pl.BlockSpec((block, shots, width), lambda i, s: (i, 0, 0))
    there = pl.BlockSpec(memory_space=pl.ANY)
    return pl.pallas_call(
        insert_kernel,
        grid_spec=pltpu.PrefetchScalarGridSpec(
            num_scalar_prefetch=1,
            grid=(rows // block,),
            in_specs=[whole(scores), whole(allowed), whole(stats), shots_spec, shots_spec, there, there],
            out_specs=pl.BlockSpec((2, lines, width), lambda i, s: (0, 0, 0)),
            scratch_shapes=[
                pltpu.VMEM((count, shots), BF16),
                pltpu.VMEM((count, shots), BF16),
                pltpu.VMEM((2, count * rows, 128), F32),
                pltpu.VMEM((count * rows, width), BF16),
                pltpu.VMEM((2, *turned.shape), BF16),
                pltpu.SemaphoreType.DMA((2,)),
            ],
        ),
        out_shape=jax.ShapeDtypeStruct((2, lines, width), BF16),
        compiler_params=pltpu.CompilerParams(
            dimension_semantics=("arbitrary",), vmem_limit_bytes=50 << 20
        ),
        name="insertion",
    )(slab, scores, allowed, stats, own, beside, turned, turned_too)


def crossed(x, axes, mask):
    return lax.ppermute(x, axes, [(i, i ^ mask) for i in range(lax.axis_size(axes))])


def combined(pairs):
    highest = jnp.max(jnp.stack([p[0] for p in pairs]), axis=0)
    total = sum(p[1] * jnp.exp(p[0] - highest) for p in pairs)
    return jnp.stack([highest, total])


def in_core_order(stats, core, shots):
    swapped = jnp.concatenate([stats[:, shots:], stats[:, :shots]], axis=1)
    return jnp.where(core == 0, stats, swapped)


def step(images, noise_weight, prior_mask, volume, interp_weights, row_first, row_count):
    owned, _, line_span = interp_weights.shape
    shots, half_rows, width = images.shape
    slab = lax.axis_index("slab")
    core = lax.axis_index("core")
    lines = volume.reshape(line_span, width)

    near = placed_rows(interp_weights, row_first, row_count, slab, half_rows)
    far = placed_rows(interp_weights, row_first, row_count, 1 - slab, half_rows)
    flat = lambda x: x.reshape(owned * half_rows, line_span)
    near, far = gathered(flat(near), flat(far))
    lines_far = shifted(lines, "slab", 1)

    beside = shifted(images, "core", 1)
    own = rows_major(images)
    beside = rows_major(beside)

    mask = prior_mask.astype(BF16)
    choose = lambda which: jnp.einsum(
        "ko,no->kn", column_choice(mask.shape[1], owned, which), mask, preferred_element_type=BF16
    )
    mask_beside = shifted(choose(1 - core), "core", 1)
    allowed = jnp.concatenate([choose(core), mask_beside], axis=1).astype(F32)

    noise_both = jnp.concatenate([noise_weight, noise_weight], axis=1)
    noise_tiled = jnp.tile(noise_both, (3, 1))
    weigh = lambda pick: weighted_slices(near[pick], far[pick], lines, lines_far, noise_tiled, half_rows)
    first, quad_first = weigh(slice(0, 4))
    second, quad_second = weigh(slice(4, 8))
    part = partial_scores(first, second, quad_first, quad_second, own, beside)
    turned = turned_weights(near[:4], far[:4])
    turned_too = turned_weights(near[4:], far[4:])
    scores = part + shifted(part, "slab", 1)

    top = jnp.max(jnp.where(allowed > 0.5, scores, -1e30), axis=0)
    mass = jnp.sum(jnp.where(allowed > 0.5, jnp.exp(scores - top[None]), 0.0), axis=0)
    pair = in_core_order(jnp.stack([top, mass]), core, shots)
    for masks in ((8, 1, 9), (2, 4, 6)):
        pair = combined([pair] + [crossed(pair, ("core", "ori"), m) for m in masks])
    pair = in_core_order(pair, core, shots)
    log_evidence = (pair[0] + jnp.log(pair[1]))[:shots]

    into = insertion(slab.reshape(1), scores, allowed, pair, own, beside, turned, turned_too)
    into = into.reshape(-1, volume.shape[1], width)
    arrived = lax.all_to_all(into, ("slab",) + IMG + ("ori",), 0, 0, tiled=True)
    inserted = jnp.sum(arrived.astype(F32), axis=0, keepdims=True)
    return log_evidence, inserted


def solution(mesh):
    torus = Mesh(
        mesh.devices.reshape(4, 2, 2, mesh.shape["ori"], mesh.shape["slab"]),
        ("y", "xh", "core", "ori", "slab"),
    )
    owner = ("ori",) + IMG
    in_specs = (
        P(IMG, "slab", None),
        P("slab", None),
        P(IMG, "ori"),
        P(None, "slab", None),
        P(owner, None, "slab"),
        P(owner, "slab"),
        P(owner, "slab"),
    )
    out_specs = (P(IMG), P(IMG + ("ori",), "slab", None))
    return jax.shard_map(step, mesh=torus, in_specs=in_specs, out_specs=out_specs, check_vma=False)
```

```python
import jax
import jax.numpy as jnp
from jax import lax
from jax.experimental import pallas as pl
from jax.experimental.pallas import tpu as pltpu
from jax.sharding import Mesh
from jax.sharding import PartitionSpec as P

IMG = ("y", "xh", "core")
BF16 = jnp.bfloat16
F32 = jnp.float32
SOURCES = ((0, 0), (0, 1), (-1, 0), (1, 0), (-1, 1), (1, 1), (2, 0), (2, 1))


def shifted(x, axis, step):
    n = lax.axis_size(axis)
    return lax.ppermute(x, axis, [(i, (i + step) % n) for i in range(n)])


def gathered(near, far):
    beside = shifted(near, "xh", 1)
    up = shifted(near, "y", 1)
    down = shifted(near, "y", -1)
    far = shifted(far, "slab", 1)
    across = shifted(up, "y", 1)
    beside_down = shifted(beside, "y", -1)
    beside_up = shifted(beside, "y", 1)
    far_beside = shifted(far, "xh", 1)
    far_down = shifted(far, "y", -1)
    far_up = shifted(far, "y", 1)
    far_across = shifted(far_down, "y", -1)
    far_beside_down = shifted(far_beside, "y", -1)
    far_beside_up = shifted(far_beside, "y", 1)
    across_beside = shifted(across, "xh", 1)
    far_across_beside = shifted(far_across, "xh", 1)
    return (
        [near, beside, up, down, beside_up, beside_down, across, across_beside],
        [far, far_beside, far_up, far_down, far_beside_up, far_beside_down, far_across, far_across_beside],
    )


def placed_rows(weights, row_first, row_count, half, half_rows):
    owned, reach, _ = weights.shape
    row = lax.broadcasted_iota(jnp.int32, (owned, half_rows, reach), 1)
    entry = lax.broadcasted_iota(jnp.int32, (owned, half_rows, reach), 2)
    at = half * half_rows + row - row_first[:, :, None]
    chosen = (entry == at) & (entry < row_count[:, :, None])
    return jnp.einsum("orj,ojl->orl", chosen.astype(BF16), weights, preferred_element_type=BF16)


def weighted_kernel(*refs):
    chips = (len(refs) - 8) // 2
    chunks = refs[: 2 * chips]
    lines, lines_far, noise, out, quad, wide, taken, done = refs[2 * chips :]
    rows = out.shape[0]
    pitch = rows + 1
    step = noise.shape[0]
    some = step // rows
    owned = chunks[0].shape[0] // rows
    fetch = lambda chip, side: pltpu.make_async_copy(
        chunks[side * chips + chip], taken.at[chip, side], done.at[chip, side]
    )
    for chip in range(chips):
        for side in range(2):
            fetch(chip, side).start()
    for chip in range(chips):
        for side in range(2):
            fetch(chip, side).wait()
        for i in range(owned // some):
            at = slice(i * step, (i + 1) * step)
            slices = jnp.dot(taken[chip, 0, at, :], lines[...], preferred_element_type=F32)
            slices += jnp.dot(taken[chip, 1, at, :], lines_far[...], preferred_element_type=F32)
            slices = slices.astype(BF16).astype(F32)
            weighted = noise[...] * slices
            first = chip * owned + i * some
            for k in range(some):
                one = weighted[k * rows : (k + 1) * rows, :]
                to = slice((first + k) * pitch, (first + k) * pitch + rows)
                wide[0, to, :] = one[:, :128]
                wide[1, to, :] = one[:, 128:]
            square = weighted * slices
            square = square[:, :128] + square[:, 128:]
            quad[first : first + some] = jnp.sum(square.reshape(some, rows // 8, 8, 128), axis=1)

    def turn(r, carry):
        for half in range(2):
            out[r, :, half * 128 : half * 128 + 128] = wide[
                half, pl.ds(r, chips * owned, stride=pitch), :
            ].astype(BF16)
        return carry

    lax.fori_loop(0, rows, turn, 0, unroll=8)


def weighted_slices(near, far, lines, lines_far, noise, rows):
    chips = len(near)
    count = chips * near[0].shape[0] // rows
    width = lines.shape[1]
    there = pl.BlockSpec(memory_space=pl.ANY)
    here = pl.BlockSpec(memory_space=pltpu.VMEM)
    return pl.pallas_call(
        weighted_kernel,
        in_specs=[there] * (2 * chips) + [here] * 3,
        out_shape=(
            jax.ShapeDtypeStruct((rows, count, width), BF16),
            jax.ShapeDtypeStruct((count, 8, 128), F32),
        ),
        scratch_shapes=[
            pltpu.VMEM((2, count * (rows + 1), 128), F32),
            pltpu.VMEM((chips, 2, *near[0].shape), BF16),
            pltpu.SemaphoreType.DMA((chips, 2)),
        ],
        compiler_params=pltpu.CompilerParams(vmem_limit_bytes=16 << 20),
        name="weighted_slices",
    )(*near, *far, lines, lines_far, noise)


def score_kernel(first, second, quad_first, quad_second, own, beside, out, acc):
    rows, shots, _ = own.shape
    block = 8
    acc[...] = jnp.zeros_like(acc)

    def add(i, carry):
        at = [i * block + r for r in range(block)]
        slices = jnp.concatenate(
            [jnp.concatenate([first[r], second[r]], axis=0) for r in at], axis=1
        )
        for k, shot in enumerate((own, beside)):
            acc[k] += lax.dot_general(
                slices,
                jnp.concatenate([shot[r] for r in at], axis=1),
                (((1,), (1,)), ((), ())),
                preferred_element_type=F32,
            )
        return carry

    lax.fori_loop(0, rows // block, add, 0)
    quad = jnp.concatenate([jnp.sum(quad_first[...], axis=1), jnp.sum(quad_second[...], axis=1)], axis=0)
    half = 0.5 * jnp.sum(quad, axis=1, keepdims=True)
    out[:, :shots] = acc[0] - half
    out[:, shots:] = acc[1] - half


def partial_scores(first, second, quad_first, quad_second, own, beside):
    _, shots, _ = own.shape
    count = first.shape[1]
    return pl.pallas_call(
        score_kernel,
        out_shape=jax.ShapeDtypeStruct((2 * count, 2 * shots), F32),
        scratch_shapes=[pltpu.VMEM((2, 2 * count, shots), F32)],
        compiler_params=pltpu.CompilerParams(vmem_limit_bytes=4 << 20),
        name="partial_scores",
    )(first, second, quad_first, quad_second, own, beside)


def rows_major_kernel(shots, out, taken, given, wide, came, went):
    total, rows, _ = shots.shape
    block = taken.shape[1]
    pitch = rows + 1
    steps = total // block
    span = lambda i: slice(i * block, (i + 1) * block)
    fetch = lambda i: pltpu.make_async_copy(shots.at[span(i)], taken.at[i % 2], came.at[i % 2])
    give = lambda i: pltpu.make_async_copy(given.at[i % 2], out.at[:, span(i), :], went.at[i % 2])
    fetch(0).start()
    for i in range(steps):
        if i + 1 < steps:
            fetch(i + 1).start()
        fetch(i).wait()

        def spread(n, carry, i=i):
            for k in range(8):
                one = taken[i % 2, n * 8 + k].astype(F32)
                at = pl.multiple_of(n * 8 * pitch, 8) + k * pitch
                wide[0, pl.ds(at, rows), :] = one[:, :128]
                wide[1, pl.ds(at, rows), :] = one[:, 128:]
            return carry

        lax.fori_loop(0, block // 8, spread, 0)
        if i >= 2:
            give(i - 2).wait()

        def turn(r, carry, i=i):
            for half in range(2):
                given[i % 2, r, :, half * 128 : half * 128 + 128] = wide[
                    half, pl.ds(r, block, stride=pitch), :
                ].astype(BF16)
            return carry

        lax.fori_loop(0, rows, turn, 0, unroll=8)
        give(i).start()
    for i in range(max(steps - 2, 0), steps):
        give(i).wait()


def rows_major(images, block=48):
    shots, rows, width = images.shape
    return pl.pallas_call(
        rows_major_kernel,
        in_specs=[pl.BlockSpec(memory_space=pl.ANY)],
        out_specs=pl.BlockSpec(memory_space=pltpu.HBM),
        out_shape=jax.ShapeDtypeStruct((rows, shots, width), BF16),
        scratch_shapes=[
            pltpu.VMEM((2, block, rows, width), BF16),
            pltpu.VMEM((2, rows, block, width), BF16),
            pltpu.VMEM((2, block * (rows + 1), 128), F32),
            pltpu.SemaphoreType.DMA((2,)),
            pltpu.SemaphoreType.DMA((2,)),
        ],
        compiler_params=pltpu.CompilerParams(vmem_limit_bytes=14 << 20),
        name="rows_major",
    )(images)


def choice_kernel(my_y, my_x, my_core, mask, kept, sent):
    shape = (kept.shape[0], mask.shape[1])
    owned = shape[0] // len(SOURCES)
    row = lax.broadcasted_iota(jnp.int32, shape, 0)
    column = lax.broadcasted_iota(jnp.int32, shape, 1)
    values = mask[...].astype(F32).astype(BF16)
    for out, core in ((kept, my_core[0]), (sent, 1 - my_core[0])):
        wanted = jnp.zeros(shape, jnp.int32)
        for at, (dy, dx) in enumerate(SOURCES):
            chip = ((my_y[0] + (dy + 4)) & 3) * 2 + ((my_x[0] + dx) & 1)
            first = (chip * 2 + core) * owned - at * owned
            wanted = jnp.where(row >= at * owned, first, wanted)
        chosen = jnp.where(column == row + wanted, 1.0, 0.0).astype(BF16)
        out[...] = lax.dot_general(
            chosen, values, (((1,), (1,)), ((), ())), preferred_element_type=F32
        ).astype(BF16)


def mask_choice(my_y, my_x, my_core, mask, count):
    shape = jax.ShapeDtypeStruct((count, mask.shape[0]), BF16)
    scalar = pl.BlockSpec(memory_space=pltpu.SMEM)
    return pl.pallas_call(
        choice_kernel,
        in_specs=[scalar] * 3 + [pl.BlockSpec(memory_space=pltpu.VMEM)],
        out_shape=(shape, shape),
        compiler_params=pltpu.CompilerParams(vmem_limit_bytes=4 << 20),
        name="mask_choice",
    )(my_y.reshape(1), my_x.reshape(1), my_core.reshape(1), mask)


def turn_kernel(*refs):
    chunks, out, flat = refs[:-2], refs[-2], refs[-1]
    half = len(chunks) // 2
    size, lines = chunks[0].shape
    for side in range(2):
        for i in range(half):
            flat[side, i * size : (i + 1) * size, :] = chunks[side * half + i][...]
    for side in range(2):

        def turn(i, carry, side=side):
            at = pl.multiple_of(i * 128, 128)
            out[side * lines : (side + 1) * lines, pl.ds(at, 128)] = flat[side, pl.ds(at, 128), :].T
            return carry

        lax.fori_loop(0, half * size // 128, turn, 0, unroll=2)


def turned_weights(near, far):
    size, lines = near[0].shape
    span = len(near) * size
    return pl.pallas_call(
        turn_kernel,
        out_shape=jax.ShapeDtypeStruct((2 * lines, span), BF16),
        scratch_shapes=[pltpu.VMEM((2, span, lines), BF16)],
        compiler_params=pltpu.CompilerParams(vmem_limit_bytes=13 << 20),
        name="turned_weights",
    )(*near, *far)


def insert_kernel(
    slab, scores, allowed, stats, own, beside, turned, turned_too, out, post_own, post_beside, wide, flat
):
    rows, shots, _ = own.shape
    pitch = rows + 1
    count = scores.shape[0]
    lines = out.shape[1]
    block = 8
    mass = jnp.exp(scores[...] - stats[0:1, :])
    post = jnp.where(allowed[...] > 0.5, mass, 0.0) / stats[1:2, :]
    post_own[...] = post[:, :shots].astype(BF16)
    post_beside[...] = post[:, shots:].astype(BF16)

    def gather(i, carry):
        for r in range(block):
            sums = jnp.dot(post_own[...], own[i * block + r], preferred_element_type=F32)
            sums += jnp.dot(post_beside[...], beside[i * block + r], preferred_element_type=F32)
            for half in range(2):
                wide[half, pl.ds(i * block + r, count, stride=pitch), :] = sums[
                    :, half * 128 : half * 128 + 128
                ]
        return carry

    lax.fori_loop(0, rows // block, gather, 0)

    def narrow(i, carry):
        for k in range(8):
            at = pl.multiple_of(i * 8 * pitch, 8) + k * pitch
            to = pl.multiple_of(i * 8 * rows, 16) + k * rows
            for half in range(2):
                flat[pl.ds(to, rows), half * 128 : half * 128 + 128] = wide[
                    half, pl.ds(at, rows), :
                ].astype(BF16)
        return carry

    lax.fori_loop(0, count // 8, narrow, 0)
    split = count * rows // 2
    for side, slot in ((0, slab[0]), (1, 1 - slab[0])):
        part = slice(side * lines, (side + 1) * lines)
        total = jnp.dot(turned[part, :], flat[:split, :], preferred_element_type=F32)
        total += jnp.dot(turned_too[part, :], flat[split:, :], preferred_element_type=F32)
        out[slot] = total.astype(BF16)


def insertion(slab, scores, allowed, stats, own, beside, turned, turned_too):
    rows, shots, width = own.shape
    count = scores.shape[0]
    lines = turned.shape[0] // 2
    return pl.pallas_call(
        insert_kernel,
        in_specs=[pl.BlockSpec(memory_space=pltpu.SMEM)]
        + [pl.BlockSpec(memory_space=pltpu.VMEM)] * 7,
        out_shape=jax.ShapeDtypeStruct((2, lines, width), BF16),
        scratch_shapes=[
            pltpu.VMEM((count, shots), BF16),
            pltpu.VMEM((count, shots), BF16),
            pltpu.VMEM((2, count * (rows + 1), 128), F32),
            pltpu.VMEM((count * rows, width), BF16),
        ],
        compiler_params=pltpu.CompilerParams(vmem_limit_bytes=14 << 20),
        name="insertion",
    )(slab, scores, allowed, stats, own, beside, turned, turned_too)


def crossed(x, axes, mask):
    return lax.ppermute(x, axes, [(i, i ^ mask) for i in range(lax.axis_size(axes))])


def combined(pairs):
    highest = jnp.max(jnp.stack([p[0] for p in pairs]), axis=0)
    total = sum(p[1] * jnp.exp(p[0] - highest) for p in pairs)
    return jnp.stack([highest, total])


def in_core_order(stats, core, shots):
    swapped = jnp.concatenate([stats[:, shots:], stats[:, :shots]], axis=1)
    return jnp.where(core == 0, stats, swapped)


def step(images, noise_weight, prior_mask, volume, interp_weights, row_first, row_count):
    owned, _, line_span = interp_weights.shape
    shots, half_rows, width = images.shape
    slab = lax.axis_index("slab")
    core = lax.axis_index("core")
    lines = volume.reshape(line_span, width)

    near = placed_rows(interp_weights, row_first, row_count, slab, half_rows)
    far = placed_rows(interp_weights, row_first, row_count, 1 - slab, half_rows)
    flat = lambda x: x.reshape(owned * half_rows, line_span)
    near, far = gathered(flat(near), flat(far))
    lines_far = shifted(lines, "slab", 1)

    beside = shifted(images, "core", 1)
    own = rows_major(images)
    beside = rows_major(beside)

    kept, sent = mask_choice(
        lax.axis_index("y"), lax.axis_index("xh"), core, prior_mask, len(SOURCES) * owned
    )
    allowed = jnp.concatenate([kept, shifted(sent, "core", 1)], axis=1).astype(F32)

    noise_both = jnp.concatenate([noise_weight, noise_weight], axis=1)
    noise_tiled = jnp.tile(noise_both, (3, 1))
    weigh = lambda pick: weighted_slices(
        near[pick], far[pick], lines, lines_far, noise_tiled, half_rows
    )
    first, quad_first = weigh(slice(0, 4))
    second, quad_second = weigh(slice(4, 8))
    part = partial_scores(first, second, quad_first, quad_second, own, beside)
    turned = turned_weights(near[:4], far[:4])
    turned_too = turned_weights(near[4:], far[4:])
    scores = part + shifted(part, "slab", 1)

    top = jnp.max(jnp.where(allowed > 0.5, scores, -1e30), axis=0)
    mass = jnp.sum(jnp.where(allowed > 0.5, jnp.exp(scores - top[None]), 0.0), axis=0)
    pair = in_core_order(jnp.stack([top, mass]), core, shots)
    for masks in ((8, 1, 9), (2, 4, 6)):
        pair = combined([pair] + [crossed(pair, ("core", "ori"), m) for m in masks])
    pair = in_core_order(pair, core, shots)
    log_evidence = (pair[0] + jnp.log(pair[1]))[:shots]

    into = insertion(slab.reshape(1), scores, allowed, pair, own, beside, turned, turned_too)
    into = into.reshape(-1, volume.shape[1], width)
    arrived = lax.all_to_all(into, ("slab",) + IMG + ("ori",), 0, 0, tiled=True)
    inserted = jnp.sum(arrived.astype(F32), axis=0, keepdims=True)
    return log_evidence, inserted


def solution(mesh):
    torus = Mesh(
        mesh.devices.reshape(4, 2, 2, mesh.shape["ori"], mesh.shape["slab"]),
        ("y", "xh", "core", "ori", "slab"),
    )
    owner = ("ori",) + IMG
    in_specs = (
        P(IMG, "slab", None),
        P("slab", None),
        P(IMG, "ori"),
        P(None, "slab", None),
        P(owner, None, "slab"),
        P(owner, "slab"),
        P(owner, "slab"),
    )
    out_specs = (P(IMG), P(IMG + ("ori",), "slab", None))
    return jax.shard_map(step, mesh=torus, in_specs=in_specs, out_specs=out_specs, check_vma=False)
```

```python
import jax
import jax.numpy as jnp
from jax import lax
from jax.experimental import pallas as pl
from jax.experimental.pallas import tpu as pltpu
from jax.sharding import Mesh
from jax.sharding import PartitionSpec as P

IMG = ("y", "xh", "core")
BF16 = jnp.bfloat16
F32 = jnp.float32
SOURCES = ((0, 0), (0, 1), (-1, 0), (1, 0), (-1, 1), (1, 1), (2, 0), (2, 1))


def shifted(x, axis, step):
    n = lax.axis_size(axis)
    return lax.ppermute(x, axis, [(i, (i + step) % n) for i in range(n)])


def gathered(near, far):
    beside = shifted(near, "xh", 1)
    up = shifted(near, "y", 1)
    down = shifted(near, "y", -1)
    far = shifted(far, "slab", 1)
    across = shifted(up, "y", 1)
    beside_down = shifted(beside, "y", -1)
    beside_up = shifted(beside, "y", 1)
    far_beside = shifted(far, "xh", 1)
    far_down = shifted(far, "y", -1)
    far_up = shifted(far, "y", 1)
    far_across = shifted(far_down, "y", -1)
    far_beside_down = shifted(far_beside, "y", -1)
    far_beside_up = shifted(far_beside, "y", 1)
    across_beside = shifted(across, "xh", 1)
    far_across_beside = shifted(far_across, "xh", 1)
    return (
        [near, beside, up, down, beside_up, beside_down, across, across_beside],
        [far, far_beside, far_up, far_down, far_beside_up, far_beside_down, far_across, far_across_beside],
    )


def placed_rows(weights, row_first, row_count, start, half_rows):
    owned, reach, _ = weights.shape
    row = lax.broadcasted_iota(jnp.int32, (owned, half_rows, reach), 1)
    entry = lax.broadcasted_iota(jnp.int32, (owned, half_rows, reach), 2)
    at = start + row - row_first[:, :, None]
    chosen = (entry == at) & (entry < row_count[:, :, None])
    return jnp.einsum("orj,ojl->orl", chosen.astype(BF16), weights, preferred_element_type=BF16)


def weighted_kernel(*refs):
    chips = (len(refs) - 6) // 2
    chunks = refs[: 2 * chips]
    lines, lines_far, noise, out, quad, wide = refs[2 * chips :]
    rows = out.shape[0]
    pitch = rows + 1
    step = noise.shape[0]
    some = step // rows
    owned = chunks[0].shape[0] // rows
    for chip in range(chips):
        for i in range(owned // some):
            at = slice(i * step, (i + 1) * step)
            slices = jnp.dot(chunks[chip][at, :], lines[...], preferred_element_type=F32)
            slices += jnp.dot(chunks[chips + chip][at, :], lines_far[...], preferred_element_type=F32)
            slices = slices.astype(BF16).astype(F32)
            weighted = noise[...] * slices
            first = chip * owned + i * some
            for k in range(some):
                one = weighted[k * rows : (k + 1) * rows, :]
                to = slice((first + k) * pitch, (first + k) * pitch + rows)
                wide[0, to, :] = one[:, :128]
                wide[1, to, :] = one[:, 128:]
            square = weighted * slices
            square = square[:, :128] + square[:, 128:]
            quad[first : first + some] = jnp.sum(square.reshape(some, rows // 8, 8, 128), axis=1)

    def turn(r, carry):
        for half in range(2):
            out[r, :, half * 128 : half * 128 + 128] = wide[
                half, pl.ds(r, chips * owned, stride=pitch), :
            ].astype(BF16)
        return carry

    lax.fori_loop(0, rows, turn, 0, unroll=8)


def weighted_slices(near, far, lines, lines_far, noise, rows):
    chips = len(near)
    count = chips * near[0].shape[0] // rows
    width = lines.shape[1]
    return pl.pallas_call(
        weighted_kernel,
        out_shape=(
            jax.ShapeDtypeStruct((rows, count, width), BF16),
            jax.ShapeDtypeStruct((count, 8, 128), F32),
        ),
        scratch_shapes=[
            pltpu.VMEM((2, count * (rows + 1), 128), F32),
        ],
        compiler_params=pltpu.CompilerParams(vmem_limit_bytes=10 << 20),
        name="weighted_slices",
    )(*near, *far, lines, lines_far, noise)


def score_kernel(first, second, quad_first, quad_second, own, beside, out, acc):
    rows, shots, _ = own.shape
    block = 8
    acc[...] = jnp.zeros_like(acc)

    def add(i, carry):
        at = [i * block + r for r in range(block)]
        slices = jnp.concatenate(
            [jnp.concatenate([first[r], second[r]], axis=0) for r in at], axis=1
        )
        for k, shot in enumerate((own, beside)):
            acc[k] += lax.dot_general(
                slices,
                jnp.concatenate([shot[r] for r in at], axis=1),
                (((1,), (1,)), ((), ())),
                preferred_element_type=F32,
            )
        return carry

    lax.fori_loop(0, rows // block, add, 0)
    quad = jnp.concatenate([jnp.sum(quad_first[...], axis=1), jnp.sum(quad_second[...], axis=1)], axis=0)
    half = 0.5 * jnp.sum(quad, axis=1, keepdims=True)
    out[:, :shots] = acc[0] - half
    out[:, shots:] = acc[1] - half


def partial_scores(first, second, quad_first, quad_second, own, beside):
    _, shots, _ = own.shape
    count = first.shape[1]
    return pl.pallas_call(
        score_kernel,
        out_shape=jax.ShapeDtypeStruct((2 * count, 2 * shots), F32),
        scratch_shapes=[pltpu.VMEM((2, 2 * count, shots), F32)],
        compiler_params=pltpu.CompilerParams(vmem_limit_bytes=4 << 20),
        name="partial_scores",
    )(first, second, quad_first, quad_second, held(own), held(beside))


def held(x, space=pltpu.VMEM):
    return pltpu.with_memory_space_constraint(x, space)


def rows_major_kernel(shots, out, taken, wide, came):
    total, rows, _ = shots.shape
    block = taken.shape[1]
    pitch = rows + 1
    steps = total // block
    span = lambda i: slice(i * block, (i + 1) * block)
    fetch = lambda i: pltpu.make_async_copy(shots.at[span(i)], taken.at[i % 2], came.at[i % 2])
    fetch(0).start()
    for i in range(steps):
        if i + 1 < steps:
            fetch(i + 1).start()
        fetch(i).wait()

        def spread(n, carry, i=i):
            for k in range(8):
                one = taken[i % 2, n * 8 + k].astype(F32)
                at = pl.multiple_of(n * 8 * pitch, 8) + k * pitch
                wide[0, pl.ds(at, rows), :] = one[:, :128]
                wide[1, pl.ds(at, rows), :] = one[:, 128:]
            return carry

        lax.fori_loop(0, block // 8, spread, 0)

        def turn(r, carry, i=i):
            for half in range(2):
                out[r, span(i), half * 128 : half * 128 + 128] = wide[
                    half, pl.ds(r, block, stride=pitch), :
                ].astype(BF16)
            return carry

        lax.fori_loop(0, rows, turn, 0, unroll=8)


def rows_major(images, block=48):
    shots, rows, width = images.shape
    return pl.pallas_call(
        rows_major_kernel,
        in_specs=[pl.BlockSpec(memory_space=pl.ANY)],
        out_specs=pl.BlockSpec(memory_space=pltpu.VMEM),
        out_shape=pltpu.VMEM((rows, shots, width), BF16),
        scratch_shapes=[
            pltpu.VMEM((2, block, rows, width), BF16),
            pltpu.VMEM((2, block * (rows + 1), 128), F32),
            pltpu.SemaphoreType.DMA((2,)),
        ],
        compiler_params=pltpu.CompilerParams(vmem_limit_bytes=9 << 20),
        name="rows_major",
    )(images)


def choice_kernel(my_y, my_x, my_core, mask, kept, sent):
    shape = (kept.shape[0], mask.shape[1])
    owned = shape[0] // len(SOURCES)
    row = lax.broadcasted_iota(jnp.int32, shape, 0)
    column = lax.broadcasted_iota(jnp.int32, shape, 1)
    values = mask[...].astype(F32).astype(BF16)
    for out, core in ((kept, my_core[0]), (sent, 1 - my_core[0])):
        wanted = jnp.zeros(shape, jnp.int32)
        for at, (dy, dx) in enumerate(SOURCES):
            chip = ((my_y[0] + (dy + 4)) & 3) * 2 + ((my_x[0] + dx) & 1)
            first = (chip * 2 + core) * owned - at * owned
            wanted = jnp.where(row >= at * owned, first, wanted)
        chosen = jnp.where(column == row + wanted, 1.0, 0.0).astype(BF16)
        out[...] = lax.dot_general(
            chosen, values, (((1,), (1,)), ((), ())), preferred_element_type=F32
        ).astype(BF16)


def mask_choice(my_y, my_x, my_core, mask, count):
    shape = jax.ShapeDtypeStruct((count, mask.shape[0]), BF16)
    scalar = pl.BlockSpec(memory_space=pltpu.SMEM)
    return pl.pallas_call(
        choice_kernel,
        in_specs=[scalar] * 3 + [pl.BlockSpec(memory_space=pltpu.VMEM)],
        out_shape=(shape, shape),
        compiler_params=pltpu.CompilerParams(vmem_limit_bytes=4 << 20),
        name="mask_choice",
    )(my_y.reshape(1), my_x.reshape(1), my_core.reshape(1), mask)


def turn_kernel(*refs):
    chunks, out, flat = refs[:-2], refs[-2], refs[-1]
    size = chunks[0].shape[0]
    for i, chunk in enumerate(chunks):
        flat[i * size : (i + 1) * size, :] = chunk[...]

    def turn(i, carry):
        at = pl.multiple_of(i * 128, 128)
        out[:, pl.ds(at, 128)] = flat[pl.ds(at, 128), :].T
        return carry

    lax.fori_loop(0, len(chunks) * size // 128, turn, 0, unroll=2)


def turned_weights(chunks):
    size, lines = chunks[0].shape
    span = len(chunks) * size
    return pl.pallas_call(
        turn_kernel,
        out_shape=pltpu.VMEM((lines, span), BF16),
        scratch_shapes=[pltpu.VMEM((span, lines), BF16)],
        compiler_params=pltpu.CompilerParams(vmem_limit_bytes=5 << 20),
        name="turned_weights",
    )(*chunks)


def insert_kernel(my_core, scores, allowed, stats, own, beside, *refs):
    turned, (out, post_own, post_beside, wide, flat) = refs[:4], refs[4:]
    rows, shots, _ = own.shape
    pitch = rows + 1
    count = scores.shape[0]
    block = 8
    mass = jnp.exp(scores[...] - stats[0:1, :])
    post = jnp.where(allowed[...] > 0.5, mass, 0.0) / stats[1:2, :]
    post_own[...] = post[:, :shots].astype(BF16)
    post_beside[...] = post[:, shots:].astype(BF16)

    def gather(i, carry):
        for r in range(block):
            sums = jnp.dot(post_own[...], own[i * block + r], preferred_element_type=F32)
            sums += jnp.dot(post_beside[...], beside[i * block + r], preferred_element_type=F32)
            for half in range(2):
                wide[half, pl.ds(i * block + r, count, stride=pitch), :] = sums[
                    :, half * 128 : half * 128 + 128
                ]
        return carry

    lax.fori_loop(0, rows // block, gather, 0)

    def narrow(i, carry):
        for k in range(8):
            at = pl.multiple_of(i * 8 * pitch, 8) + k * pitch
            to = pl.multiple_of(i * 8 * rows, 16) + k * rows
            for half in range(2):
                flat[pl.ds(to, rows), half * 128 : half * 128 + 128] = wide[
                    half, pl.ds(at, rows), :
                ].astype(BF16)
        return carry

    lax.fori_loop(0, count // 8, narrow, 0)
    split = count * rows // 2
    for side in range(2):
        total = jnp.dot(turned[side][...], flat[:split, :], preferred_element_type=F32)
        total += jnp.dot(turned[2 + side][...], flat[split:, :], preferred_element_type=F32)
        lines, width = total.shape
        parts = total.reshape(8, 2, lines // 16, width)
        for other in range(2):
            mine = jnp.where(my_core[0] == other, parts[:, 0], parts[:, 1])
            out[2 * other + side] = mine.reshape(lines // 2, width).astype(BF16)


def insertion(my_core, scores, allowed, stats, own, beside, turned):
    rows, shots, width = own.shape
    count = scores.shape[0]
    lines = turned[0].shape[0]
    return pl.pallas_call(
        insert_kernel,
        in_specs=[pl.BlockSpec(memory_space=pltpu.SMEM)]
        + [pl.BlockSpec(memory_space=pltpu.VMEM)] * 9,
        out_shape=jax.ShapeDtypeStruct((4, lines // 2, width), BF16),
        scratch_shapes=[
            pltpu.VMEM((count, shots), BF16),
            pltpu.VMEM((count, shots), BF16),
            pltpu.VMEM((2, count * (rows + 1), 128), F32),
            pltpu.VMEM((count * rows, width), BF16),
        ],
        compiler_params=pltpu.CompilerParams(vmem_limit_bytes=14 << 20),
        name="insertion",
    )(my_core.reshape(1), scores, allowed, stats, held(own), held(beside), *map(held, turned))


def crossed(x, axes, mask):
    return lax.ppermute(x, axes, [(i, i ^ mask) for i in range(lax.axis_size(axes))])


def combined(pairs):
    highest = jnp.max(jnp.stack([p[0] for p in pairs]), axis=0)
    total = sum(p[1] * jnp.exp(p[0] - highest) for p in pairs)
    return jnp.stack([highest, total])


def in_core_order(stats, first_core, shots):
    swapped = jnp.concatenate([stats[:, shots:], stats[:, :shots]], axis=1)
    return jnp.where(first_core, stats, swapped)


def step(images, noise_weight, prior_mask, volume, interp_weights, row_first, row_count):
    owned, _, line_span = interp_weights.shape
    shots, half_rows, width = images.shape
    slab = lax.axis_index("slab")
    core = lax.axis_index("core")
    interp_weights, lines, near_at, far_at, my_y, my_x, core, first_core = lax.optimization_barrier(
        (
            interp_weights,
            volume.reshape(line_span, width),
            slab * half_rows,
            (1 - slab) * half_rows,
            lax.axis_index("y"),
            lax.axis_index("xh"),
            core,
            core == 0,
        )
    )

    near = placed_rows(interp_weights, row_first, row_count, near_at, half_rows)
    far = placed_rows(interp_weights, row_first, row_count, far_at, half_rows)
    flat = lambda x: x.reshape(owned * half_rows, line_span)
    near, far = gathered(flat(near), flat(far))
    lines_far = shifted(lines, "slab", 1)

    beside = shifted(images, "core", 1)
    own = rows_major(held(images, pltpu.HBM))
    beside = rows_major(beside)

    kept, sent = mask_choice(my_y, my_x, core, prior_mask, len(SOURCES) * owned)
    allowed = jnp.concatenate([kept, shifted(sent, "core", 1)], axis=1).astype(F32)

    noise_both = jnp.concatenate([noise_weight, noise_weight], axis=1)
    noise_tiled = jnp.tile(noise_both, (3, 1))
    weigh = lambda pick: weighted_slices(
        near[pick], far[pick], lines, lines_far, noise_tiled, half_rows
    )
    first, quad_first = weigh(slice(0, 4))
    second, quad_second = weigh(slice(4, 8))
    part = partial_scores(first, second, quad_first, quad_second, own, beside)
    turned = [
        turned_weights(near[:4]),
        turned_weights(far[:4]),
        turned_weights(near[4:]),
        turned_weights(far[4:]),
    ]
    scores = part + shifted(part, "slab", 1)

    top = jnp.max(jnp.where(allowed > 0.5, scores, -1e30), axis=0)
    mass = jnp.sum(jnp.where(allowed > 0.5, jnp.exp(scores - top[None]), 0.0), axis=0)
    pair = in_core_order(jnp.stack([top, mass]), first_core, shots)
    for masks in ((8, 1, 9), (2, 4, 6)):
        pair = combined([pair] + [crossed(pair, ("core", "ori"), m) for m in masks])
    pair = in_core_order(pair, first_core, shots)
    log_evidence = (pair[0] + jnp.log(pair[1]))[:shots]

    into = insertion(core, scores, allowed, pair, own, beside, turned)
    square = into[0].astype(F32)
    for m in range(1, 4):
        square += crossed(into[m], ("core", "slab"), m).astype(F32)
    square = square.astype(BF16).reshape(-1, volume.shape[1], width)
    arrived = lax.all_to_all(square, ("y", "xh", "ori"), 0, 0, tiled=True)
    inserted = jnp.sum(arrived.astype(F32), axis=0, keepdims=True)
    return log_evidence, inserted


def solution(mesh):
    torus = Mesh(
        mesh.devices.reshape(4, 2, 2, mesh.shape["ori"], mesh.shape["slab"]),
        ("y", "xh", "core", "ori", "slab"),
    )
    owner = ("ori",) + IMG
    in_specs = (
        P(IMG, "slab", None),
        P("slab", None),
        P(IMG, "ori"),
        P(None, "slab", None),
        P(owner, None, "slab"),
        P(owner, "slab"),
        P(owner, "slab"),
    )
    out_specs = (P(IMG), P(IMG + ("ori",), "slab", None))
    return jax.shard_map(step, mesh=torus, in_specs=in_specs, out_specs=out_specs, check_vma=False)
```

```python
import jax
import jax.numpy as jnp
from jax import lax
from jax.experimental import pallas as pl
from jax.experimental.pallas import tpu as pltpu
from jax.sharding import Mesh
from jax.sharding import PartitionSpec as P

IMG = ("y", "xh", "core")
BF16 = jnp.bfloat16
F32 = jnp.float32
SOURCES = ((0, 0), (0, 1), (-1, 0), (1, 0), (-1, 1), (1, 1), (2, 0), (2, 1))


ROUNDS = ((3, 2, 1), (14, 6, 8))


def shifted(x, axis, step):
    n = lax.axis_size(axis)
    return lax.ppermute(x, axis, [(i, (i + step) % n) for i in range(n)])


def gathered(near, far):
    beside = shifted(near, "xh", 1)
    up = shifted(near, "y", 1)
    down = shifted(near, "y", -1)
    far = shifted(far, "slab", 1)
    across = shifted(up, "y", 1)
    beside_down = shifted(beside, "y", -1)
    beside_up = shifted(beside, "y", 1)
    far_beside = shifted(far, "xh", 1)
    far_down = shifted(far, "y", -1)
    far_up = shifted(far, "y", 1)
    middle = far_down.shape[0] // 2
    far_across = shifted(far_down[:middle], "y", -1)
    far_across_too = shifted(far_down[middle:], "y", -1)
    far_beside_down = shifted(far_beside, "y", -1)
    far_beside_up = shifted(far_beside, "y", 1)
    across_beside = shifted(across, "xh", 1)
    far_across_beside = shifted(far_across, "xh", 1)
    far_across_beside_too = shifted(far_across_too, "xh", 1)
    return (
        [near, beside, up, down, beside_up, beside_down, across, across_beside],
        [far, far_beside, far_up, far_down, far_beside_up, far_beside_down]
        + [far_across, far_across_too, far_across_beside, far_across_beside_too],
    )


def placed_rows(weights, row_first, row_count, start, half_rows):
    owned, reach, _ = weights.shape
    row = lax.broadcasted_iota(jnp.int32, (owned, half_rows, reach), 1)
    entry = lax.broadcasted_iota(jnp.int32, (owned, half_rows, reach), 2)
    at = start + row - row_first[:, :, None]
    chosen = (entry == at) & (entry < row_count[:, :, None])
    return jnp.einsum("orj,ojl->orl", chosen.astype(BF16), weights, preferred_element_type=BF16)


def weighted_kernel(*refs):
    *chunks, lines, lines_far, noise, out, quad, wide = refs
    rows = out.shape[0]
    pitch = rows + 1
    step = noise.shape[0]
    some = step // rows
    count = quad.shape[0]
    pieces = [(c, slice(i, i + step)) for c in chunks for i in range(0, c.shape[0], step)]
    half = len(pieces) // 2
    for i, ((near, at), (far, far_at)) in enumerate(zip(pieces[:half], pieces[half:])):
        slices = jnp.dot(near[at, :], lines[...], preferred_element_type=F32)
        slices += jnp.dot(far[far_at, :], lines_far[...], preferred_element_type=F32)
        slices = slices.astype(BF16).astype(F32)
        weighted = noise[...] * slices
        first = i * some
        for k in range(some):
            one = weighted[k * rows : (k + 1) * rows, :]
            to = slice((first + k) * pitch, (first + k) * pitch + rows)
            wide[0, to, :] = one[:, :128]
            wide[1, to, :] = one[:, 128:]
        square = weighted * slices
        square = square[:, :128] + square[:, 128:]
        quad[first : first + some] = jnp.sum(square.reshape(some, rows // 8, 8, 128), axis=1)

    def turn(r, carry):
        for half in range(2):
            out[r, :, half * 128 : half * 128 + 128] = wide[
                half, pl.ds(r, count, stride=pitch), :
            ].astype(BF16)
        return carry

    lax.fori_loop(0, rows, turn, 0, unroll=8)


def weighted_slices(near, far, lines, lines_far, noise, rows):
    count = sum(x.shape[0] for x in near) // rows
    width = lines.shape[1]
    return pl.pallas_call(
        weighted_kernel,
        out_shape=(
            jax.ShapeDtypeStruct((rows, count, width), BF16),
            jax.ShapeDtypeStruct((count, 8, 128), F32),
        ),
        scratch_shapes=[
            pltpu.VMEM((2, count * (rows + 1), 128), F32),
        ],
        compiler_params=pltpu.CompilerParams(vmem_limit_bytes=10 << 20),
        name="weighted_slices",
    )(*near, *far, lines, lines_far, noise)


def score_kernel(first, second, quad_first, quad_second, own, beside, out, acc):
    rows, shots, _ = own.shape
    block = 8
    acc[...] = jnp.zeros_like(acc)

    def add(i, carry):
        at = [i * block + r for r in range(block)]
        slices = jnp.concatenate(
            [jnp.concatenate([first[r], second[r]], axis=0) for r in at], axis=1
        )
        for k, shot in enumerate((own, beside)):
            acc[k] += lax.dot_general(
                slices,
                jnp.concatenate([shot[r] for r in at], axis=1),
                (((1,), (1,)), ((), ())),
                preferred_element_type=F32,
            )
        return carry

    lax.fori_loop(0, rows // block, add, 0)
    quad = jnp.concatenate([jnp.sum(quad_first[...], axis=1), jnp.sum(quad_second[...], axis=1)], axis=0)
    half = 0.5 * jnp.sum(quad, axis=1, keepdims=True)
    out[:, :shots] = acc[0] - half
    out[:, shots:] = acc[1] - half


def partial_scores(first, second, quad_first, quad_second, own, beside):
    _, shots, _ = own.shape
    count = first.shape[1]
    return pl.pallas_call(
        score_kernel,
        out_shape=jax.ShapeDtypeStruct((2 * count, 2 * shots), F32),
        scratch_shapes=[pltpu.VMEM((2, 2 * count, shots), F32)],
        compiler_params=pltpu.CompilerParams(vmem_limit_bytes=4 << 20),
        name="partial_scores",
    )(first, second, quad_first, quad_second, held(own), held(beside))


def held(x, space=pltpu.VMEM):
    return pltpu.with_memory_space_constraint(x, space)


def rows_major_kernel(shots, out, taken, wide, came):
    total, rows, _ = shots.shape
    block = taken.shape[1]
    pitch = rows + 1
    steps = total // block
    span = lambda i: slice(i * block, (i + 1) * block)
    fetch = lambda i: pltpu.make_async_copy(shots.at[span(i)], taken.at[i % 2], came.at[i % 2])
    fetch(0).start()
    for i in range(steps):
        if i + 1 < steps:
            fetch(i + 1).start()
        fetch(i).wait()

        def spread(n, carry, i=i):
            for k in range(8):
                one = taken[i % 2, n * 8 + k].astype(F32)
                at = pl.multiple_of(n * 8 * pitch, 8) + k * pitch
                wide[0, pl.ds(at, rows), :] = one[:, :128]
                wide[1, pl.ds(at, rows), :] = one[:, 128:]
            return carry

        lax.fori_loop(0, block // 8, spread, 0)

        def turn(r, carry, i=i):
            for half in range(2):
                out[r, span(i), half * 128 : half * 128 + 128] = wide[
                    half, pl.ds(r, block, stride=pitch), :
                ].astype(BF16)
            return carry

        lax.fori_loop(0, rows, turn, 0, unroll=8)


def rows_major(images, block=48):
    shots, rows, width = images.shape
    return pl.pallas_call(
        rows_major_kernel,
        in_specs=[pl.BlockSpec(memory_space=pl.ANY)],
        out_specs=pl.BlockSpec(memory_space=pltpu.VMEM),
        out_shape=pltpu.VMEM((rows, shots, width), BF16),
        scratch_shapes=[
            pltpu.VMEM((2, block, rows, width), BF16),
            pltpu.VMEM((2, block * (rows + 1), 128), F32),
            pltpu.SemaphoreType.DMA((2,)),
        ],
        compiler_params=pltpu.CompilerParams(vmem_limit_bytes=9 << 20),
        name="rows_major",
    )(images)


def choice_kernel(my_y, my_x, my_core, mask, kept, sent):
    shape = (kept.shape[0], mask.shape[1])
    owned = shape[0] // len(SOURCES)
    row = lax.broadcasted_iota(jnp.int32, shape, 0)
    column = lax.broadcasted_iota(jnp.int32, shape, 1)
    values = mask[...].astype(F32).astype(BF16)
    for out, core in ((kept, my_core[0]), (sent, 1 - my_core[0])):
        wanted = jnp.zeros(shape, jnp.int32)
        for at, (dy, dx) in enumerate(SOURCES):
            chip = ((my_y[0] + (dy + 4)) & 3) * 2 + ((my_x[0] + dx) & 1)
            first = (chip * 2 + core) * owned - at * owned
            wanted = jnp.where(row >= at * owned, first, wanted)
        chosen = jnp.where(column == row + wanted, 1.0, 0.0).astype(BF16)
        out[...] = lax.dot_general(
            chosen, values, (((1,), (1,)), ((), ())), preferred_element_type=F32
        ).astype(BF16)


def mask_choice(my_y, my_x, my_core, mask, count):
    shape = jax.ShapeDtypeStruct((count, mask.shape[0]), BF16)
    scalar = pl.BlockSpec(memory_space=pltpu.SMEM)
    return pl.pallas_call(
        choice_kernel,
        in_specs=[scalar] * 3 + [pl.BlockSpec(memory_space=pltpu.VMEM)],
        out_shape=(shape, shape),
        compiler_params=pltpu.CompilerParams(vmem_limit_bytes=4 << 20),
        name="mask_choice",
    )(my_y.reshape(1), my_x.reshape(1), my_core.reshape(1), mask)


def turn_kernel(*refs):
    *chunks, out, flat = refs
    at = 0
    for chunk in chunks:
        flat[at : at + chunk.shape[0], :] = chunk[...]
        at += chunk.shape[0]

    def turn(i, carry):
        at = pl.multiple_of(i * 128, 128)
        out[:, pl.ds(at, 128)] = flat[pl.ds(at, 128), :].T
        return carry

    lax.fori_loop(0, flat.shape[0] // 128, turn, 0, unroll=2)


def turned_weights(chunks):
    span = sum(x.shape[0] for x in chunks)
    lines = chunks[0].shape[1]
    return pl.pallas_call(
        turn_kernel,
        out_shape=pltpu.VMEM((lines, span), BF16),
        scratch_shapes=[pltpu.VMEM((span, lines), BF16)],
        compiler_params=pltpu.CompilerParams(vmem_limit_bytes=5 << 20),
        name="turned_weights",
    )(*chunks)


def insert_kernel(my_core, scores, allowed, stats, own, beside, *refs):
    turned, (out, post_own, post_beside, wide, flat) = refs[:4], refs[4:]
    rows, shots, _ = own.shape
    pitch = rows + 1
    count = scores.shape[0]
    block = 8
    mass = jnp.exp(scores[...] - stats[0:1, :])
    post = jnp.where(allowed[...] > 0.5, mass, 0.0) / stats[1:2, :]
    post_own[...] = post[:, :shots].astype(BF16)
    post_beside[...] = post[:, shots:].astype(BF16)

    def gather(i, carry):
        for r in range(block):
            sums = jnp.dot(post_own[...], own[i * block + r], preferred_element_type=F32)
            sums += jnp.dot(post_beside[...], beside[i * block + r], preferred_element_type=F32)
            for half in range(2):
                wide[half, pl.ds(i * block + r, count, stride=pitch), :] = sums[
                    :, half * 128 : half * 128 + 128
                ]
        return carry

    lax.fori_loop(0, rows // block, gather, 0)

    def narrow(i, carry):
        for k in range(8):
            at = pl.multiple_of(i * 8 * pitch, 8) + k * pitch
            to = pl.multiple_of(i * 8 * rows, 16) + k * rows
            for half in range(2):
                flat[pl.ds(to, rows), half * 128 : half * 128 + 128] = wide[
                    half, pl.ds(at, rows), :
                ].astype(BF16)
        return carry

    lax.fori_loop(0, count // 8, narrow, 0)
    split = count * rows // 2
    for side in range(2):
        total = jnp.dot(turned[side][...], flat[:split, :], preferred_element_type=F32)
        total += jnp.dot(turned[2 + side][...], flat[split:, :], preferred_element_type=F32)
        lines, width = total.shape
        parts = total.reshape(8, 2, lines // 16, width)
        for other in range(2):
            mine = jnp.where(my_core[0] == other, parts[:, 0], parts[:, 1])
            out[2 * other + side] = mine.reshape(lines // 2, width).astype(BF16)


def insertion(my_core, scores, allowed, stats, own, beside, turned):
    rows, shots, width = own.shape
    count = scores.shape[0]
    lines = turned[0].shape[0]
    return pl.pallas_call(
        insert_kernel,
        in_specs=[pl.BlockSpec(memory_space=pltpu.SMEM)]
        + [pl.BlockSpec(memory_space=pltpu.VMEM)] * 9,
        out_shape=jax.ShapeDtypeStruct((4, lines // 2, width), BF16),
        scratch_shapes=[
            pltpu.VMEM((count, shots), BF16),
            pltpu.VMEM((count, shots), BF16),
            pltpu.VMEM((2, count * (rows + 1), 128), F32),
            pltpu.VMEM((count * rows, width), BF16),
        ],
        compiler_params=pltpu.CompilerParams(vmem_limit_bytes=14 << 20),
        name="insertion",
    )(my_core.reshape(1), scores, allowed, stats, held(own), held(beside), *map(held, turned))


def crossed(x, axes, mask):
    return lax.ppermute(x, axes, [(i, i ^ mask) for i in range(lax.axis_size(axes))])


def combined(pairs):
    highest = jnp.max(jnp.stack([p[0] for p in pairs]), axis=0)
    total = sum(p[1] * jnp.exp(p[0] - highest) for p in pairs)
    return jnp.stack([highest, total])


def in_core_order(stats, first_core, shots):
    swapped = jnp.concatenate([stats[:, shots:], stats[:, :shots]], axis=1)
    return jnp.where(first_core, stats, swapped)


def step(images, noise_weight, prior_mask, volume, interp_weights, row_first, row_count):
    owned, _, line_span = interp_weights.shape
    shots, half_rows, width = images.shape
    slab = lax.axis_index("slab")
    core = lax.axis_index("core")
    interp_weights, lines, near_at, far_at, my_y, my_x, core, first_core = lax.optimization_barrier(
        (
            interp_weights,
            volume.reshape(line_span, width),
            slab * half_rows,
            (1 - slab) * half_rows,
            lax.axis_index("y"),
            lax.axis_index("xh"),
            core,
            core == 0,
        )
    )

    near = placed_rows(interp_weights, row_first, row_count, near_at, half_rows)
    far = placed_rows(interp_weights, row_first, row_count, far_at, half_rows)
    flat = lambda x: x.reshape(owned * half_rows, line_span)
    near, far = gathered(flat(near), flat(far))
    lines_far = shifted(lines, "slab", 1)

    beside = shifted(images, "core", 1)
    own = rows_major(held(images, pltpu.HBM))
    beside = rows_major(beside)

    kept, sent = mask_choice(my_y, my_x, core, prior_mask, len(SOURCES) * owned)
    allowed = jnp.concatenate([kept, shifted(sent, "core", 1)], axis=1).astype(F32)

    noise_both = jnp.concatenate([noise_weight, noise_weight], axis=1)
    noise_tiled = jnp.tile(noise_both, (3, 1))
    weigh = lambda pick: weighted_slices(
        near[pick], far[pick], lines, lines_far, noise_tiled, half_rows
    )
    first, quad_first = weigh(slice(0, 4))
    second, quad_second = weigh(slice(4, None))
    part = partial_scores(first, second, quad_first, quad_second, own, beside)
    turned = [
        turned_weights(near[:4]),
        turned_weights(far[:4]),
        turned_weights(near[4:]),
        turned_weights(far[4:]),
    ]
    scores = part + shifted(part, "slab", 1)

    top = jnp.max(jnp.where(allowed > 0.5, scores, -1e30), axis=0)
    mass = jnp.sum(jnp.where(allowed > 0.5, jnp.exp(scores - top[None]), 0.0), axis=0)
    pair = in_core_order(jnp.stack([top, mass]), first_core, shots)
    for masks in ROUNDS:
        pair = combined([pair] + [crossed(pair, ("core", "ori"), m) for m in masks])
    pair = in_core_order(pair, first_core, shots)
    log_evidence = (pair[0] + jnp.log(pair[1]))[:shots]

    into = insertion(core, scores, allowed, pair, own, beside, turned)
    square = into[0].astype(F32)
    for m in range(1, 4):
        square += crossed(into[m], ("core", "slab"), m).astype(F32)
    square = square.astype(BF16).reshape(-1, volume.shape[1], width)
    arrived = lax.all_to_all(square, ("y", "xh", "ori"), 0, 0, tiled=True)
    inserted = jnp.sum(arrived.astype(F32), axis=0, keepdims=True)
    return log_evidence, inserted


def solution(mesh):
    torus = Mesh(
        mesh.devices.reshape(4, 2, 2, mesh.shape["ori"], mesh.shape["slab"]),
        ("y", "xh", "core", "ori", "slab"),
    )
    owner = ("ori",) + IMG
    in_specs = (
        P(IMG, "slab", None),
        P("slab", None),
        P(IMG, "ori"),
        P(None, "slab", None),
        P(owner, None, "slab"),
        P(owner, "slab"),
        P(owner, "slab"),
    )
    out_specs = (P(IMG), P(IMG + ("ori",), "slab", None))
    return jax.shard_map(step, mesh=torus, in_specs=in_specs, out_specs=out_specs, check_vma=False)
```
